32 devices in a mesh: dp: 4 (over y, x), expert: 8 (over z, core).
Axes of the slice: x: 2, y: 2, z: 4, core: 2. Of those that a mesh axis runs over, the one named last changes fastest.
Arguments:
- master: float32 [2, 32, 64, 2880], P(None, 'expert', 'dp'), may hold values from -6 to 6
- moment_one: float32 [2, 32, 64, 2880], P(None, 'expert', 'dp'), may hold values from -1.2 to 1.2
- moment_two: float32 [2, 32, 64, 2880], P(None, 'expert', 'dp'), may hold values from 0.0005 to 0.5
- gradient: bfloat16 [2, 32, 64, 2880], P(None, 'expert', 'dp'), may hold values from -150000 to 150000
- old_slot: int32 [2, 32], replicated, may hold values from 0 to 31, as said below
- new_slot: int32 [2, 32], replicated, may hold values from 0 to 31, as said below
Outputs:
- new_master: float32 [2, 32, 64, 2880], P(None, 'expert', 'dp')
- new_moment_one: float32 [2, 32, 64, 2880], P(None, 'expert', 'dp')
- new_moment_two: float32 [2, 32, 64, 2880], P(None, 'expert', 'dp')
The draws below stay inside these ranges and needn't reach their ends.
Inputs may be any that keep to these rules, and one draw needn't show every extreme that they name: `old_slot`: for each layer a permutation of 0 to 31; global slot s is held by index s // 4 of expert. `new_slot`: for each layer a permutation of 0 to 31; in each layer exactly 1 slot of each index of expert receives another expert than it held, and exactly 1 of the experts held by each index leaves its slot; all other experts keep their slot.
All inputs are finite; a program needn't handle non-finite values.
Results may differ from the reference program's by a relative error of at most 0.001.
Values sent between devices are 32-bit elements; how exact they have to be, the bound alone decides.
A program may use at most 64 MiB of HBM per device.

```python
import math
import jax
import jax.numpy as jnp
from jax import lax

D = 2880
EXP_DEV = 4
EXPERTS = 32
RROWS = 64
LAYERS = 2
MOVE_DEV = 1


def placement_pair(key):
    base_key = jax.random.fold_in(key, 17)
    group_size = EXPERTS // EXP_DEV
    old_tables = []
    new_tables = []
    for layer_index in range(LAYERS):
        layer_key = jax.random.fold_in(base_key, layer_index)
        key_perm, key_pick, key_cycle = jax.random.split(layer_key, 3)
        old_layer = jax.random.permutation(key_perm, EXPERTS).astype(jnp.int32)
        scores = jax.random.randint(key_pick, (group_size, EXP_DEV), 0, 1 << 20, dtype=jnp.int32) * EXP_DEV
        scores = scores + lax.broadcasted_iota(jnp.int32, (group_size, EXP_DEV), 1)
        chosen = jnp.argsort(scores, axis=1)[:, :MOVE_DEV].astype(jnp.int32)
        chosen = (chosen + lax.broadcasted_iota(jnp.int32, chosen.shape, 0) * EXP_DEV).reshape(-1)
        cycle_order = jax.random.permutation(key_cycle, group_size * MOVE_DEV).astype(jnp.int32)
        ordered = chosen[cycle_order]
        destination = jnp.arange(EXPERTS, dtype=jnp.int32).at[ordered].set(jnp.roll(ordered, -1))
        old_tables.append(old_layer)
        new_tables.append(destination[old_layer].astype(jnp.int32))
    return (jnp.stack(old_tables), jnp.stack(new_tables))


def draw_old_slot(key, part):
    return placement_pair(key)[0]


def draw_new_slot(key, part):
    return placement_pair(key)[1]


def draw_gradient(key, part):
    key_noise = jax.random.fold_in(jax.random.fold_in(key, 29), 0)
    key_row = jax.random.fold_in(jax.random.fold_in(key, 29), 1)
    key_col = jax.random.fold_in(jax.random.fold_in(key, 29), 2)
    key_block = jax.random.fold_in(jax.random.fold_in(key, 29), 4)
    key_total = jax.random.fold_in(jax.random.fold_in(key, 29), 5)
    full_shape = (LAYERS, EXPERTS, RROWS, D)
    slot_place = lax.broadcasted_iota(jnp.float32, (1, EXPERTS, 1, 1), 1) / (EXPERTS - 1)
    block_scale = jnp.exp(jax.random.uniform(key_block, (LAYERS, EXPERTS, 1, 1), jnp.float32, 0.0, math.log(2.0)))
    total_scale = jnp.exp(jax.random.uniform(key_total, (), jnp.float32, 0.0, math.log(4.0)))
    slot_rise = 1.0 + 2.0 * slot_place
    noise = jax.random.normal(key_noise, full_shape, jnp.float32)
    row_scale = jnp.exp(jax.random.uniform(key_row, (LAYERS, EXPERTS, RROWS, 1), jnp.float32, 0.0, math.log(10.0)))
    col_scale = jnp.exp(jax.random.uniform(key_col, (LAYERS, 1, 1, D), jnp.float32, 0.0, math.log(10.0)))
    return (noise * row_scale * col_scale * slot_rise * block_scale * total_scale).astype(jnp.bfloat16)


def steps_of(own_key, extent, cuts, smallest, high):
    def one(dim, shards_of):
        heights = jax.random.uniform(jax.random.fold_in(jax.random.fold_in(own_key, 6), dim), (shards_of,), jnp.float32, smallest / len(cuts), high / len(cuts))
        return jnp.repeat(jnp.exp(heights), extent[dim] // shards_of).reshape((-1,) + (1,) * (len(extent) - dim - 1))

    gain = one(*cuts[0])
    for cut in cuts[1:]:
        gain = gain * one(*cut)
    return gain


def gaussian(stream_key, dims, scale, reach, cuts=(), kind=jnp.bfloat16):
    array = scale * jax.random.normal(stream_key, dims, jnp.float32)
    if cuts:
        array = array * steps_of(stream_key, dims, cuts, -0.22, 0.18)
    return jnp.clip(array, -reach, reach).astype(kind)


def setup_inputs(seed: int = 0) -> dict:
    key_of = jax.random.split(jax.random.key(seed), 7)
    return {
        "master": gaussian(key_of[0], (LAYERS, EXPERTS, RROWS, D), 1.0, 6.0, ((1, 8), (2, 4)), jnp.float32),
        "moment_one": gaussian(key_of[1], (LAYERS, EXPERTS, RROWS, D), 0.2, 1.2, ((1, 8), (2, 4)), jnp.float32),
        "moment_two": jnp.clip(jnp.exp(math.log(0.5) - 6.9077552 * jax.random.uniform(key_of[2], (LAYERS, EXPERTS, RROWS, D), jnp.float32) ** steps_of(key_of[2], (LAYERS, EXPERTS, RROWS, D), ((1, 8), (2, 4)), -0.2, 0.2)), 0.0005, 0.5),
        "gradient": draw_gradient(jax.random.fold_in(key_of[6], 71), 0),
        "old_slot": draw_old_slot(jax.random.fold_in(key_of[6], 71), 0),
        "new_slot": draw_new_slot(jax.random.fold_in(key_of[6], 71), 0),
    }


BETA_ONE = 0.9
BETA_TWO = 0.95
LEARN_RATE = 0.05
DECAY_RATE = 0.1
ADAM_EPS = 1e-08
CLIP_RMS = 2.0
FIRST_FIX = 1.0 - 0.9 ** 10
SECOND_FIX = 1.0 - 0.95 ** 10

def adam_update(master, moment_one, moment_two, gradient, clip_scale):
    scaled = gradient.astype(jnp.float32) * clip_scale
    first_moment = BETA_ONE * moment_one + (1.0 - BETA_ONE) * scaled
    second = BETA_TWO * moment_two + (1.0 - BETA_TWO) * scaled * scaled
    step_dir = first_moment / FIRST_FIX / (jnp.sqrt(second / SECOND_FIX) + ADAM_EPS)
    weights = master - LEARN_RATE * (step_dir + DECAY_RATE * master)
    return (weights, first_moment, second)

def clip_factor(square_sum, entry_count):
    return jnp.minimum(1.0, CLIP_RMS * math.sqrt(entry_count) / (jnp.sqrt(square_sum) + 1e-06))

def pick_rows(data, chosen):
    return jax.vmap(lambda layer_block, layer_pick: jnp.take(layer_block, layer_pick, axis=0))(data, chosen)

def reference(master, moment_one, moment_two, gradient, old_slot, new_slot):
    widened = gradient.astype(jnp.float32)
    square_sum = jnp.sum(widened * widened)
    clip_scale = clip_factor(square_sum, LAYERS * EXPERTS * RROWS * D)
    updated = adam_update(master, moment_one, moment_two, gradient, clip_scale)
    holder = jnp.argsort(new_slot, axis=1).astype(jnp.int32)
    source = jnp.take_along_axis(old_slot, holder, axis=1).astype(jnp.int32)
    return (pick_rows(updated[0], source), pick_rows(updated[1], source), pick_rows(updated[2], source))
```

```python
import functools
import math

import jax
import jax.numpy as jnp
from jax import lax
from jax.experimental import pallas as pl
from jax.experimental.pallas import tpu as pltpu
from jax.sharding import PartitionSpec as P

MESH = pl.DeviceIdType.MESH
BETA_ONE = 0.9
BETA_TWO = 0.95
LEARN_RATE = 0.05
DECAY_RATE = 0.1
ADAM_EPS = 1e-08
CLIP_RMS = 2.0
FIRST_FIX = 1.0 - 0.9**10
SECOND_FIX = 1.0 - 0.95**10
SUB, LANE = 8, 128


def moments(moment_one, moment_two, gradient, clip_scale):
    scaled = gradient * clip_scale
    first_moment = BETA_ONE * moment_one + (1.0 - BETA_ONE) * scaled
    second = BETA_TWO * moment_two + (1.0 - BETA_TWO) * scaled * scaled
    return first_moment, second


def weights_of(master, first_moment, second):
    step_dir = first_moment / FIRST_FIX / (jnp.sqrt(second / SECOND_FIX) + ADAM_EPS)
    return master - LEARN_RATE * (step_dir + DECAY_RATE * master)


def plan_kernel(group, slots, old_ref, new_ref, mine_ref, send_ref, pick_ref, count_ref, dst_ref, src_ref, rank_ref):
    layers, experts = old_ref.shape
    half = group // 2
    me = lax.axis_index("expert")
    my_half = lax.div(me, half)

    def clear(i, c):
        send_ref[i] = 0
        return c

    lax.fori_loop(0, layers * half, clear, 0)
    for layer in range(layers):

        def expert_step(e, c):
            old, new = old_ref[layer, e], new_ref[layer, e]

            @pl.when(old != new)
            def _():
                src, dst = lax.div(old, slots), lax.div(new, slots)
                dst_ref[layer * group + src] = dst
                src_ref[layer * group + dst] = src

                @pl.when(src == me)
                def _():
                    mine_ref[layer] = lax.rem(old, slots)

                @pl.when(dst == me)
                def _():
                    mine_ref[layers + layer] = lax.rem(new, slots)

            return c

        lax.fori_loop(0, experts, expert_step, 0)
    counts = [jnp.int32(0), jnp.int32(0)]
    for layer in range(layers):
        for side in range(2):

            def rank_step(j, count, side=side):
                at = layer * group + side * half + j
                crosses = lax.div(dst_ref[at], half) != side
                rank_ref[at] = count

                @pl.when(crosses & (my_half == side))
                def _():
                    send_ref[count] = layer * half + j

                return count + crosses.astype(jnp.int32)

            counts[side] = lax.fori_loop(0, half, rank_step, counts[side])
    count_ref[0] = counts[0]
    for layer in range(layers):

        def pick_step(j, c):
            src = src_ref[layer * group + my_half * half + j]
            local = lax.div(src, half) == my_half
            pick_ref[layer * half + j] = jnp.where(
                local,
                layer * half + lax.rem(src, half),
                layers * half + rank_ref[layer * group + src],
            )
            return c

        lax.fori_loop(0, half, pick_step, 0)


def make_plan(old_slot, new_slot, group, slots):
    layers = old_slot.shape[0]
    half = group // 2
    smem = pl.BlockSpec(memory_space=pltpu.SMEM)
    i32 = lambda n: jax.ShapeDtypeStruct((n,), jnp.int32)
    return pl.pallas_call(
        functools.partial(plan_kernel, group, slots),
        out_shape=(i32(2 * layers), i32(layers * half), i32(layers * half), i32(1)),
        in_specs=[smem, smem],
        out_specs=(smem, smem, smem, smem),
        scratch_shapes=[pltpu.SMEM((layers * group,), jnp.int32)] * 3,
    )(old_slot, new_slot)


def move_kernel(
    dims, mine_ref, send_ref, pick_ref, master_ref, one_ref, two_ref, grad_ref,
    land0, land1, land2, clip_ref,
    src0, src1, src2, hub0, hub1, hub2, far0, far1, far2, out0, out1, out2, give0, give1, give2,
    norm_dp, norm_ex, norm_a, norm_b,
    a_send, a_recv, b_send, b_recv, c_send, c_recv, d_send, d_recv, e_send, e_recv,
):
    group, dps, layers, slots, rows, cols, tiles, piece, cap = dims
    half, hubs = group // 2, group // 4
    lands, srcs, hubbuf = (land0, land1, land2), (src0, src1, src2), (hub0, hub1, hub2)
    fars, outs, gives = (far0, far1, far2), (out0, out1, out2), (give0, give1, give2)
    me, my_dp = lax.axis_index("expert"), lax.axis_index("dp")
    my_half = lax.div(me, half)
    base = my_half * half
    spot = lax.rem(me, half)
    first_hub = hubs + my_half * hubs
    is_hub = (me >= hubs) & (me < 3 * hubs)
    my_piece = lax.rem(me, hubs)
    partner = jnp.where(my_half == 0, me + hubs, me - hubs)
    col_tiles = -(-cols // LANE)

    def place(ref, layer, block):
        for r in range(rows // SUB):
            for c in range(col_tiles):
                tile = block[r * SUB:(r + 1) * SUB, c * LANE:min((c + 1) * LANE, cols)]
                if tile.shape[1] < LANE:
                    tile = jnp.concatenate(
                        [tile, jnp.zeros((SUB, LANE - tile.shape[1]), jnp.float32)], axis=1
                    )
                ref[layer, r * col_tiles + c] = tile

    for layer in range(layers):
        place(src0, layer, master_ref[layer, mine_ref[layer]])
        for s in (src0, src1, src2):
            for t in range(tiles, piece * hubs):
                s[layer, t] = jnp.zeros((SUB, LANE), jnp.float32)

    barrier = pltpu.get_barrier_semaphore()

    def greet(d, c):
        @pl.when(d != me)
        def _():
            pl.semaphore_signal(barrier, inc=1, device_id={"expert": d}, device_id_type=MESH)

        return c

    def greet_dp(d, c):
        @pl.when(d != my_dp)
        def _():
            pl.semaphore_signal(barrier, inc=1, device_id={"dp": d}, device_id_type=MESH)

        return c

    lax.fori_loop(0, group, greet, 0)
    lax.fori_loop(0, dps, greet_dp, 0)
    pl.semaphore_wait(barrier, group + dps - 2)

    def a_copy(a, layer, p, slot):
        return pltpu.make_async_remote_copy(
            src_ref=srcs[a].at[layer, pl.ds(p * piece, piece)],
            dst_ref=hubbuf[a].at[layer * half + slot],
            send_sem=a_send.at[a, layer, p],
            recv_sem=a_recv.at[a, layer * half + slot],
            device_id={"expert": first_hub + p},
            device_id_type=MESH,
        )

    def a_start(a):
        for layer in range(layers):
            for p in range(hubs):
                mine = first_hub + p == me

                @pl.when(jnp.logical_not(mine))
                def _(layer=layer, p=p):
                    a_copy(a, layer, p, spot).start()

                @pl.when(mine)
                def _(layer=layer, p=p):
                    hubbuf[a][layer * half + spot] = srcs[a][layer, p * piece:(p + 1) * piece]

    def a_wait_send(a):
        for layer in range(layers):
            for p in range(hubs):

                @pl.when(first_hub + p != me)
                def _(layer=layer, p=p):
                    a_copy(a, layer, p, spot).wait_send()

    def a_wait_recv(a):
        for layer in range(layers):

            def step(j, c, layer=layer):
                @pl.when(j != spot)
                def _():
                    a_copy(a, layer, 0, j).wait_recv()

                return c

            lax.fori_loop(0, half, step, 0)

    def b_copy(a):
        return pltpu.make_async_remote_copy(
            src_ref=outs[a], dst_ref=fars[a], send_sem=b_send.at[a], recv_sem=b_recv.at[a],
            device_id={"expert": partner}, device_id_type=MESH,
        )

    def b_start(a):
        def step(k, c):
            outs[a][k] = hubbuf[a][send_ref[k]]
            return c

        lax.fori_loop(0, cap, step, 0)
        b_copy(a).start()

    def c_copy(a, layer, j, p):
        return pltpu.make_async_remote_copy(
            src_ref=gives[a].at[layer * half + j],
            dst_ref=lands[a].at[layer, pl.ds(p * piece, piece)],
            send_sem=c_send.at[a, layer * half + j],
            recv_sem=c_recv.at[a, layer, p],
            device_id={"expert": base + j},
            device_id_type=MESH,
        )

    def c_start(a):
        for layer in range(layers):

            def step(j, c, layer=layer):
                code = pick_ref[layer * half + j]
                near = hubbuf[a][jnp.minimum(code, layers * half - 1)]
                far = fars[a][jnp.clip(code - layers * half, 0, cap - 1)]
                chosen = jnp.where(code < layers * half, near, far)

                @pl.when(j != spot)
                def _():
                    gives[a][layer * half + j] = chosen
                    c_copy(a, layer, j, my_piece).start()

                @pl.when(j == spot)
                def _():
                    lands[a][layer, pl.ds(my_piece * piece, piece)] = chosen

                return c

            lax.fori_loop(0, half, step, 0)

    def c_wait_send(a):
        for layer in range(layers):

            def step(j, c, layer=layer):
                @pl.when(j != spot)
                def _():
                    c_copy(a, layer, j, my_piece).wait_send()

                return c

            lax.fori_loop(0, half, step, 0)

    def c_wait_recv(a):
        for layer in range(layers):
            for p in range(hubs):

                @pl.when(first_hub + p != me)
                def _(layer=layer, p=p):
                    c_copy(a, layer, 0, p).wait_recv()

    a_start(0)

    acc = jnp.zeros((rows, cols), jnp.float32)
    for layer in range(layers):
        for s in range(slots):
            wide = grad_ref[layer, s].astype(jnp.float32)
            acc = acc + wide * wide

    def exchange(value, send_buf, box, axis, size, mine, send_sem, recv_sem):
        tile = jnp.full((SUB, LANE), value, jnp.float32)
        send_buf[...] = tile
        box[mine] = tile

        def copy(peer, slot):
            return pltpu.make_async_remote_copy(
                src_ref=send_buf, dst_ref=box.at[slot], send_sem=send_sem.at[peer],
                recv_sem=recv_sem.at[slot], device_id={axis: peer}, device_id_type=MESH,
            )

        def each(act):
            def step(d, c):
                @pl.when(d != mine)
                def _():
                    act(d)

                return c

            lax.fori_loop(0, size, step, 0)

        each(lambda d: copy(d, mine).start())
        each(lambda d: copy(d, d).wait_recv())
        each(lambda d: copy(d, mine).wait_send())
        total = box[0]
        for d in range(1, size):
            total = total + box[d]
        return total

    by_dp = exchange(jnp.sum(acc), norm_a, norm_dp, "dp", dps, my_dp, d_send, d_recv)
    total = exchange(by_dp, norm_b, norm_ex, "expert", group, me, e_send, e_recv)
    entry_count = layers * slots * group * rows * dps * cols
    clip = jnp.minimum(1.0, CLIP_RMS * math.sqrt(entry_count) / (jnp.sqrt(total) + 1e-06))
    clip_ref[...] = clip
    scale = clip[0:1, 0:1]
    for layer in range(layers):
        slot = mine_ref[layer]
        first, second = moments(
            one_ref[layer, slot], two_ref[layer, slot],
            grad_ref[layer, slot].astype(jnp.float32), scale,
        )
        place(src1, layer, first)
        place(src2, layer, second)
    a_start(1)
    a_start(2)

    @pl.when(is_hub)
    def _():
        a_wait_recv(0)
        b_start(0)
        a_wait_recv(1)
        b_start(1)
        b_copy(0).wait_recv()
        c_start(0)
        a_wait_recv(2)
        b_start(2)
        b_copy(1).wait_recv()
        c_start(1)
        b_copy(2).wait_recv()
        c_start(2)
        for a in range(3):
            b_copy(a).wait_send()
            c_wait_send(a)

    for a in range(3):
        a_wait_send(a)
        c_wait_recv(a)


def move_blocks(plan, master, moment_one, moment_two, gradient, group, dps, cap):
    mine, send, pick = plan
    layers, slots, rows, cols = master.shape
    half, hubs = group // 2, group // 4
    tiles = (rows // SUB) * -(-cols // LANE)
    piece = -(-tiles // hubs)
    dims = (group, dps, layers, slots, rows, cols, tiles, piece, cap)
    smem = pl.BlockSpec(memory_space=pltpu.SMEM)
    vmem = pl.BlockSpec(memory_space=pltpu.VMEM)
    f32 = jnp.float32
    buf = lambda *lead: pltpu.VMEM(lead + (SUB, LANE), f32)
    dma = lambda *shape: pltpu.SemaphoreType.DMA(shape)
    land = jax.ShapeDtypeStruct((layers, piece * hubs, SUB, LANE), f32)
    return pl.pallas_call(
        functools.partial(move_kernel, dims),
        out_shape=(land, land, land, jax.ShapeDtypeStruct((SUB, LANE), f32)),
        in_specs=[smem] * 3 + [vmem] * 4,
        out_specs=(vmem,) * 4,
        scratch_shapes=[buf(layers, piece * hubs)] * 3
        + [buf(layers * half, piece)] * 3
        + [buf(cap, piece)] * 3
        + [buf(cap, piece)] * 3
        + [buf(layers * half, piece)] * 3
        + [buf(dps), buf(group), buf(), buf()]
        + [dma(3, layers, hubs), dma(3, layers * half), dma(3), dma(3), dma(3, layers * half),
           dma(3, layers, hubs), dma(dps), dma(dps), dma(group), dma(group)],
        compiler_params=pltpu.CompilerParams(
            collective_id=cap, has_side_effects=True, vmem_limit_bytes=48 * 1024 * 1024
        ),
    )(mine, send, pick, master, moment_one, moment_two, gradient)


def merge_kernel(mine_ref, master_ref, one_ref, two_ref, grad_ref, land0, land1, land2, clip_ref, w_ref, f_ref, s_ref):
    layer, slot = pl.program_id(0), pl.program_id(1)
    layers = pl.num_programs(0)
    rows, cols = w_ref.shape[2:]
    arrives = mine_ref[layers + layer] == slot

    @pl.when(jnp.logical_not(arrives))
    def _():
        first, second = moments(
            one_ref[0, 0], two_ref[0, 0], grad_ref[0, 0].astype(jnp.float32), clip_ref[0:1, 0:1]
        )
        f_ref[0, 0] = first
        s_ref[0, 0] = second
        w_ref[0, 0] = weights_of(master_ref[0, 0], first, second)

    @pl.when(arrives)
    def _():
        col_tiles = -(-cols // LANE)
        for r in range(rows // SUB):
            for c in range(col_tiles):
                t = r * col_tiles + c
                width = min(LANE, cols - c * LANE)
                at = (0, 0, pl.ds(r * SUB, SUB), pl.ds(c * LANE, width))
                first, second = land1[0, t][:, :width], land2[0, t][:, :width]
                f_ref[at] = first
                s_ref[at] = second
                w_ref[at] = weights_of(land0[0, t][:, :width], first, second)


def merge(mine, master, moment_one, moment_two, gradient, landed, clip):
    layers, slots, rows, cols = master.shape
    own = pl.BlockSpec((1, 1, rows, cols), lambda l, s, m: (l, s, 0, 0))
    came = pl.BlockSpec((1,) + landed[0].shape[1:], lambda l, s, m: (l, 0, 0, 0))
    out = jax.ShapeDtypeStruct(master.shape, jnp.float32)
    return pl.pallas_call(
        merge_kernel,
        out_shape=(out, out, out),
        grid_spec=pltpu.PrefetchScalarGridSpec(
            num_scalar_prefetch=1,
            grid=(layers, slots),
            in_specs=[own] * 4 + [came] * 3 + [pl.BlockSpec((SUB, LANE), lambda l, s, m: (0, 0))],
            out_specs=(own, own, own),
        ),
    )(mine, master, moment_one, moment_two, gradient, *landed, clip)


def shards(group, dps, master, moment_one, moment_two, gradient, old_slot, new_slot):
    layers, slots = master.shape[:2]
    mine, send, pick, count = make_plan(old_slot, new_slot, group, slots)
    *landed, clip = move_blocks(
        (mine, send, pick), master, moment_one, moment_two, gradient, group, dps, layers * (group // 2)
    )
    return merge(mine, master, moment_one, moment_two, gradient, landed, clip)


def solution(mesh):
    split = P(None, "expert", "dp", None)
    body = functools.partial(shards, mesh.shape["expert"], mesh.shape["dp"])
    return jax.shard_map(
        body, mesh=mesh, in_specs=(split,) * 4 + (P(), P()), out_specs=(split,) * 3, check_vma=False
    )
```

```python
import functools
import math

import jax
import jax.numpy as jnp
from jax import lax
from jax.experimental import pallas as pl
from jax.experimental.pallas import tpu as pltpu
from jax.sharding import PartitionSpec as P

MESH = pl.DeviceIdType.MESH
BETA_ONE = 0.9
BETA_TWO = 0.95
LEARN_RATE = 0.05
DECAY_RATE = 0.1
ADAM_EPS = 1e-08
CLIP_RMS = 2.0
FIRST_FIX = 1.0 - 0.9**10
SECOND_FIX = 1.0 - 0.95**10
SUB, LANE = 8, 128


def moments(moment_one, moment_two, gradient, clip_scale):
    scaled = gradient * clip_scale
    first_moment = BETA_ONE * moment_one + (1.0 - BETA_ONE) * scaled
    second = BETA_TWO * moment_two + (1.0 - BETA_TWO) * scaled * scaled
    return first_moment, second


def weights_of(master, first_moment, second):
    step_dir = first_moment / FIRST_FIX / (jnp.sqrt(second / SECOND_FIX) + ADAM_EPS)
    return master - LEARN_RATE * (step_dir + DECAY_RATE * master)


def plan_kernel(group, slots, levels, old_ref, new_ref, mine_ref, send_ref, pick_ref, count_ref, dst_ref, src_ref, rank_ref):
    layers, experts = old_ref.shape
    half = group // 2
    me = lax.axis_index("expert")
    my_half = lax.div(me, half)

    def clear(i, c):
        send_ref[i] = 0
        return c

    lax.fori_loop(0, layers * half, clear, 0)
    for layer in range(layers):

        def expert_step(e, c):
            old, new = old_ref[layer, e], new_ref[layer, e]

            @pl.when(old != new)
            def _():
                src, dst = lax.div(old, slots), lax.div(new, slots)
                dst_ref[layer * group + src] = dst
                src_ref[layer * group + dst] = src

                @pl.when(src == me)
                def _():
                    mine_ref[layer] = lax.rem(old, slots)

                @pl.when(dst == me)
                def _():
                    mine_ref[layers + layer] = lax.rem(new, slots)

            return c

        lax.fori_loop(0, experts, expert_step, 0)
    counts = [jnp.int32(0), jnp.int32(0)]
    for layer in range(layers):
        for side in range(2):

            def rank_step(j, count, side=side):
                at = layer * group + side * half + j
                crosses = lax.div(dst_ref[at], half) != side
                rank_ref[at] = count

                @pl.when(crosses & (my_half == side))
                def _():
                    send_ref[count] = layer * half + j

                return count + crosses.astype(jnp.int32)

            counts[side] = lax.fori_loop(0, half, rank_step, counts[side])
    count_ref[0] = sum((counts[0] > level).astype(jnp.int32) for level in levels[:-1])
    for layer in range(layers):

        def pick_step(j, c):
            src = src_ref[layer * group + my_half * half + j]
            local = lax.div(src, half) == my_half
            pick_ref[layer * half + j] = jnp.where(
                local,
                layer * half + lax.rem(src, half),
                layers * half + rank_ref[layer * group + src],
            )
            return c

        lax.fori_loop(0, half, pick_step, 0)


def make_plan(old_slot, new_slot, group, slots, levels):
    layers = old_slot.shape[0]
    half = group // 2
    smem = pl.BlockSpec(memory_space=pltpu.SMEM)
    i32 = lambda n: jax.ShapeDtypeStruct((n,), jnp.int32)
    return pl.pallas_call(
        functools.partial(plan_kernel, group, slots, levels),
        out_shape=(i32(2 * layers), i32(layers * half), i32(layers * half), i32(1)),
        in_specs=[smem, smem],
        out_specs=(smem, smem, smem, smem),
        scratch_shapes=[pltpu.SMEM((layers * group,), jnp.int32)] * 3,
    )(old_slot, new_slot)


def move_kernel(
    dims, mine_ref, send_ref, pick_ref, master_hbm, one_hbm, two_hbm, grad_hbm,
    land0, land1, land2, clip_ref, master_ref, one_ref, two_ref, grad_ref, src0, src1, src2,
    norm_dp, norm_ex, norm_a, norm_b, in_sem,
    a_send, a_recv, b_send, b_recv, c_send, c_recv, d_send, d_recv, e_send, e_recv, *bufs,
):
    group, dps, layers, slots, rows, cols, tiles, cuts, cap = dims
    half, hubs = group // 2, group // 4
    piece = cuts[-1]
    chunks = [(a, lo, hi) for a in range(3) for lo, hi in zip(cuts[:-1], cuts[1:])]
    count = len(chunks)
    hubbuf, fars, outs, gives = (bufs[i * count:(i + 1) * count] for i in range(4))
    lands, srcs = (land0, land1, land2), (src0, src1, src2)
    me, my_dp = lax.axis_index("expert"), lax.axis_index("dp")
    my_half = lax.div(me, half)
    base = my_half * half
    spot = lax.rem(me, half)
    first_hub = hubs + my_half * hubs
    is_hub = (me >= hubs) & (me < 3 * hubs)
    my_piece = lax.rem(me, hubs)
    partner = jnp.where(my_half == 0, me + hubs, me - hubs)
    col_tiles = -(-cols // LANE)

    loads = [
        pltpu.make_async_copy(src, dst, in_sem.at[i])
        for i, (src, dst) in enumerate(
            ((master_hbm, master_ref), (grad_hbm, grad_ref), (one_hbm, one_ref), (two_hbm, two_ref))
        )
    ]
    for load in loads:
        load.start()

    barrier = pltpu.get_barrier_semaphore()

    def greet(d, c):
        @pl.when(d != me)
        def _():
            pl.semaphore_signal(barrier, inc=1, device_id={"expert": d}, device_id_type=MESH)

        return c

    def greet_dp(d, c):
        @pl.when(d != my_dp)
        def _():
            pl.semaphore_signal(barrier, inc=1, device_id={"dp": d}, device_id_type=MESH)

        return c

    lax.fori_loop(0, group, greet, 0)
    lax.fori_loop(0, dps, greet_dp, 0)

    def padded(tile):
        if tile.shape[1] == LANE:
            return tile
        return jnp.concatenate([tile, jnp.zeros((SUB, LANE - tile.shape[1]), jnp.float32)], axis=1)

    def spans():
        for r in range(rows // SUB):
            for c in range(col_tiles):
                yield r * col_tiles + c, pl.ds(r * SUB, SUB), pl.ds(c * LANE, min(LANE, cols - c * LANE))

    loads[0].wait()
    for layer in range(layers):
        slot = mine_ref[layer]
        for t, rspan, cspan in spans():
            src0[layer, t] = padded(master_ref[layer, slot, rspan, cspan])
        for s in srcs:
            for t in range(tiles, piece * hubs):
                s[layer, t] = jnp.zeros((SUB, LANE), jnp.float32)

    pl.semaphore_wait(barrier, group + dps - 2)

    def a_copy(n, layer, p, slot):
        a, lo, hi = chunks[n]
        return pltpu.make_async_remote_copy(
            src_ref=srcs[a].at[layer, pl.ds(p * piece + lo, hi - lo)],
            dst_ref=hubbuf[n].at[layer * half + slot],
            send_sem=a_send.at[n, layer, p],
            recv_sem=a_recv.at[n, layer * half + slot],
            device_id={"expert": first_hub + p},
            device_id_type=MESH,
        )

    def a_start(n):
        a, lo, hi = chunks[n]
        for layer in range(layers):
            for p in range(hubs):
                mine = first_hub + p == me

                @pl.when(jnp.logical_not(mine))
                def _(layer=layer, p=p):
                    a_copy(n, layer, p, spot).start()

                @pl.when(mine)
                def _(layer=layer, p=p):
                    hubbuf[n][layer * half + spot] = srcs[a][layer, p * piece + lo:p * piece + hi]

    def a_wait_send(n):
        for layer in range(layers):
            for p in range(hubs):

                @pl.when(first_hub + p != me)
                def _(layer=layer, p=p):
                    a_copy(n, layer, p, spot).wait_send()

    def a_wait_recv(n):
        for layer in range(layers):

            def step(j, c, layer=layer):
                @pl.when(j != spot)
                def _():
                    a_copy(n, layer, 0, j).wait_recv()

                return c

            lax.fori_loop(0, half, step, 0)

    def b_copy(n):
        return pltpu.make_async_remote_copy(
            src_ref=outs[n], dst_ref=fars[n], send_sem=b_send.at[n], recv_sem=b_recv.at[n],
            device_id={"expert": partner}, device_id_type=MESH,
        )

    def b_start(n):
        def step(k, c):
            outs[n][k] = hubbuf[n][send_ref[k]]
            return c

        lax.fori_loop(0, cap, step, 0)
        b_copy(n).start()

    def landing(n, layer, p):
        a, lo, hi = chunks[n]
        return lands[a].at[layer, pl.ds(p * piece + lo, hi - lo)]

    def c_copy(n, layer, j, p):
        return pltpu.make_async_remote_copy(
            src_ref=gives[n].at[layer * half + j],
            dst_ref=landing(n, layer, p),
            send_sem=c_send.at[n, layer * half + j],
            recv_sem=c_recv.at[n, layer, p],
            device_id={"expert": base + j},
            device_id_type=MESH,
        )

    def c_start(n):
        for layer in range(layers):

            def step(j, c, layer=layer):
                code = pick_ref[layer * half + j]
                near = hubbuf[n][jnp.minimum(code, layers * half - 1)]
                far = fars[n][jnp.clip(code - layers * half, 0, cap - 1)]
                gives[n][layer * half + j] = jnp.where(code < layers * half, near, far)
                return c

            lax.fori_loop(0, half, step, 0)

        for layer in range(layers):

            def send(j, c, layer=layer):
                @pl.when(j != spot)
                def _():
                    c_copy(n, layer, j, my_piece).start()

                return c

            lax.fori_loop(0, half, send, 0)
            landing(n, layer, my_piece)[...] = gives[n][layer * half + spot]

    def c_wait_send(n):
        for layer in range(layers):

            def step(j, c, layer=layer):
                @pl.when(j != spot)
                def _():
                    c_copy(n, layer, j, my_piece).wait_send()

                return c

            lax.fori_loop(0, half, step, 0)

    def c_wait_recv(n):
        for layer in range(layers):
            for p in range(hubs):

                @pl.when(first_hub + p != me)
                def _(layer=layer, p=p):
                    c_copy(n, layer, 0, p).wait_recv()

    early = [n for n in range(count) if chunks[n][0] == 0]
    for n in early:
        a_start(n)

    loads[1].wait()
    parts = [jnp.zeros((rows, LANE), jnp.float32) for _ in range(4)]
    tails = jnp.zeros((rows, cols - (col_tiles - 1) * LANE), jnp.float32)
    for layer in range(layers):
        for s in range(slots):
            for c in range(col_tiles - 1):
                wide = grad_ref[layer, s, :, pl.ds(c * LANE, LANE)].astype(jnp.float32)
                parts[c % 4] = parts[c % 4] + wide * wide
            last = (col_tiles - 1) * LANE
            wide = grad_ref[layer, s, :, pl.ds(last, cols - last)].astype(jnp.float32)
            tails = tails + wide * wide
    square = jnp.sum((parts[0] + parts[1]) + (parts[2] + parts[3])) + jnp.sum(tails)

    def exchange(value, send_buf, box, axis, size, mine, send_sem, recv_sem):
        tile = jnp.full((SUB, LANE), value, jnp.float32)
        send_buf[...] = tile
        box[mine] = tile

        def copy(peer, slot):
            return pltpu.make_async_remote_copy(
                src_ref=send_buf, dst_ref=box.at[slot], send_sem=send_sem.at[peer],
                recv_sem=recv_sem.at[slot], device_id={axis: peer}, device_id_type=MESH,
            )

        def each(act):
            def step(d, c):
                @pl.when(d != mine)
                def _():
                    act(d)

                return c

            lax.fori_loop(0, size, step, 0)

        each(lambda d: copy(d, mine).start())
        each(lambda d: copy(d, d).wait_recv())
        each(lambda d: copy(d, mine).wait_send())
        total = box[0]
        for d in range(1, size):
            total = total + box[d]
        return total

    by_dp = exchange(square, norm_a, norm_dp, "dp", dps, my_dp, d_send, d_recv)
    total = exchange(by_dp, norm_b, norm_ex, "expert", group, me, e_send, e_recv)
    entry_count = layers * slots * group * rows * dps * cols
    clip = jnp.minimum(1.0, CLIP_RMS * math.sqrt(entry_count) / (jnp.sqrt(total) + 1e-06))
    clip_ref[...] = clip
    loads[2].wait()
    loads[3].wait()
    for layer in range(layers):
        slot = mine_ref[layer]
        for c in range(col_tiles):
            cspan = pl.ds(c * LANE, min(LANE, cols - c * LANE))
            wide = grad_ref[layer, slot, :, cspan].astype(jnp.float32)
            first, second = moments(
                one_ref[layer, slot, :, cspan], two_ref[layer, slot, :, cspan], wide, clip[0:1, 0:1]
            )
            for r in range(rows // SUB):
                src1[layer, r * col_tiles + c] = padded(first[r * SUB:(r + 1) * SUB])
                src2[layer, r * col_tiles + c] = padded(second[r * SUB:(r + 1) * SUB])
    for n in range(len(early), count):
        a_start(n)

    @pl.when(is_hub)
    def _():
        for n in range(count):
            a_wait_recv(n)
            b_start(n)
            if n:
                b_copy(n - 1).wait_recv()
                c_start(n - 1)
        b_copy(count - 1).wait_recv()
        c_start(count - 1)
        for n in range(count):
            b_copy(n).wait_send()
            c_wait_send(n)

    for n in range(count):
        a_wait_send(n)
        c_wait_recv(n)


def move_blocks(group, dps, cap, ident, mine, send, pick, master, moment_one, moment_two, gradient):
    layers, slots, rows, cols = master.shape
    half, hubs = group // 2, group // 4
    tiles = (rows // SUB) * -(-cols // LANE)
    piece = -(-tiles // hubs)
    cuts = (0, piece // 2, piece)
    dims = (group, dps, layers, slots, rows, cols, tiles, cuts, cap)
    smem = pl.BlockSpec(memory_space=pltpu.SMEM)
    hbm = pl.BlockSpec(memory_space=pltpu.HBM)
    vmem = pl.BlockSpec(memory_space=pltpu.VMEM)
    f32 = jnp.float32
    buf = lambda *lead: pltpu.VMEM(lead + (SUB, LANE), f32)
    dma = lambda *shape: pltpu.SemaphoreType.DMA(shape)
    land = jax.ShapeDtypeStruct((layers, piece * hubs, SUB, LANE), f32)
    widths = [hi - lo for lo, hi in zip(cuts[:-1], cuts[1:])] * 3
    count = len(widths)
    return pl.pallas_call(
        functools.partial(move_kernel, dims),
        out_shape=(land, land, land, jax.ShapeDtypeStruct((SUB, LANE), f32)),
        in_specs=[smem] * 3 + [hbm] * 4,
        out_specs=(vmem,) * 4,
        scratch_shapes=[pltpu.VMEM(master.shape, f32)] * 3
        + [pltpu.VMEM(gradient.shape, gradient.dtype)]
        + [buf(layers, piece * hubs)] * 3
        + [buf(dps), buf(group), buf(), buf()]
        + [dma(4)]
        + [dma(count, layers, hubs), dma(count, layers * half), dma(count), dma(count),
           dma(count, layers * half), dma(count, layers, hubs), dma(dps), dma(dps), dma(group), dma(group)]
        + [buf(layers * half, w) for w in widths]
        + [buf(cap, w) for w in widths] * 2
        + [buf(layers * half, w) for w in widths],
        compiler_params=pltpu.CompilerParams(
            collective_id=ident, has_side_effects=True, vmem_limit_bytes=40 * 1024 * 1024
        ),
    )(mine, send, pick, master, moment_one, moment_two, gradient)


def merge_kernel(
    mine_ref, master_hbm, one_hbm, two_hbm, grad_hbm, came0, came1, came2, clip_ref, w_hbm, f_hbm, s_hbm,
    master_ref, one_ref, two_ref, grad_ref, w_ref, f_ref, s_ref, in_sem, out_sem,
):
    layers, slots, rows, cols = master_ref.shape
    col_tiles = -(-cols // LANE)
    pairs = ((grad_hbm, grad_ref), (one_hbm, one_ref), (two_hbm, two_ref), (master_hbm, master_ref))
    blocks = layers * slots

    def read(i, n):
        layer, slot = lax.div(i, slots), lax.rem(i, slots)
        src, dst = pairs[n]
        return pltpu.make_async_copy(src.at[layer, slot], dst.at[layer, slot], in_sem.at[i, n])

    def write(i, n):
        layer, slot = lax.div(i, slots), lax.rem(i, slots)
        src, dst = ((w_ref, w_hbm), (f_ref, f_hbm), (s_ref, s_hbm))[n]
        return pltpu.make_async_copy(src.at[layer, slot], dst.at[layer, slot], out_sem.at[i, n])

    def begin(i, c):
        for n in range(4):
            read(i, n).start()
        return c

    lax.fori_loop(0, blocks, begin, 0)

    def step(i, c):
        layer, slot = lax.div(i, slots), lax.rem(i, slots)
        for n in range(4):
            read(i, n).wait()

        arrives = mine_ref[layers + layer] == slot

        @pl.when(jnp.logical_not(arrives))
        def _():
            scale = clip_ref[0:1, 0:1]
            for k in range(col_tiles):
                at = (layer, slot, slice(None), pl.ds(k * LANE, min(LANE, cols - k * LANE)))
                first, second = moments(one_ref[at], two_ref[at], grad_ref[at].astype(jnp.float32), scale)
                f_ref[at] = first
                s_ref[at] = second
                w_ref[at] = weights_of(master_ref[at], first, second)

        @pl.when(arrives)
        def _():
            for r in range(rows // SUB):
                for k in range(col_tiles):
                    t = r * col_tiles + k
                    width = min(LANE, cols - k * LANE)
                    at = (layer, slot, pl.ds(r * SUB, SUB), pl.ds(k * LANE, width))
                    first, second = came1[layer, t][:, :width], came2[layer, t][:, :width]
                    f_ref[at] = first
                    s_ref[at] = second
                    w_ref[at] = weights_of(came0[layer, t][:, :width], first, second)

        for n in range(3):
            write(i, n).start()
        return c

    lax.fori_loop(0, blocks, step, 0)

    def end(i, c):
        for n in range(3):
            write(i, n).wait()
        return c

    lax.fori_loop(0, blocks, end, 0)


def merge(mine, master, moment_one, moment_two, gradient, landed, clip):
    layers, slots = master.shape[:2]
    blocks = layers * slots
    smem = pl.BlockSpec(memory_space=pltpu.SMEM)
    hbm = pl.BlockSpec(memory_space=pltpu.HBM)
    vmem = pl.BlockSpec(memory_space=pltpu.VMEM)
    full = pltpu.VMEM(master.shape, jnp.float32)
    out = jax.ShapeDtypeStruct(master.shape, jnp.float32)
    dma = lambda *shape: pltpu.SemaphoreType.DMA(shape)
    return pl.pallas_call(
        merge_kernel,
        out_shape=(out, out, out),
        in_specs=[smem] + [hbm] * 4 + [vmem] * 4,
        out_specs=(hbm,) * 3,
        scratch_shapes=[full] * 3
        + [pltpu.VMEM(gradient.shape, gradient.dtype)]
        + [full] * 3
        + [dma(blocks, 4), dma(blocks, 3)],
        compiler_params=pltpu.CompilerParams(vmem_limit_bytes=40 * 1024 * 1024),
    )(mine, master, moment_one, moment_two, gradient, *landed, clip)


def shards(group, dps, master, moment_one, moment_two, gradient, old_slot, new_slot):
    layers, slots = master.shape[:2]
    full = layers * (group // 2)
    levels = sorted({-(-full * step // 8) for step in range(1, 9)})
    mine, send, pick, index = make_plan(old_slot, new_slot, group, slots, levels)
    moves = [
        functools.partial(move_blocks, group, dps, level, ident) for ident, level in enumerate(levels)
    ]
    *landed, clip = lax.switch(
        index[0], moves, mine, send, pick, master, moment_one, moment_two, gradient
    )
    return merge(mine, master, moment_one, moment_two, gradient, landed, clip)


def solution(mesh):
    split = P(None, "expert", "dp", None)
    body = functools.partial(shards, mesh.shape["expert"], mesh.shape["dp"])
    return jax.shard_map(
        body, mesh=mesh, in_specs=(split,) * 4 + (P(), P()), out_specs=(split,) * 3, check_vma=False
    )
```

```python
import functools
import math

import jax
import jax.numpy as jnp
from jax import lax
from jax.experimental import pallas as pl
from jax.experimental.pallas import tpu as pltpu
from jax.sharding import PartitionSpec as P

MESH = pl.DeviceIdType.MESH
BETA_ONE = 0.9
BETA_TWO = 0.95
LEARN_RATE = 0.05
DECAY_RATE = 0.1
ADAM_EPS = 1e-08
CLIP_RMS = 2.0
FIRST_FIX = 1.0 - 0.9**10
SECOND_FIX = 1.0 - 0.95**10
SUB, LANE = 8, 128


def moments(moment_one, moment_two, gradient, clip_scale):
    scaled = gradient * clip_scale
    first_moment = BETA_ONE * moment_one + (1.0 - BETA_ONE) * scaled
    second = BETA_TWO * moment_two + (1.0 - BETA_TWO) * scaled * scaled
    return first_moment, second


def weights_of(master, first_moment, second):
    step_dir = first_moment / FIRST_FIX / (jnp.sqrt(second / SECOND_FIX) + ADAM_EPS)
    return master - LEARN_RATE * (step_dir + DECAY_RATE * master)


def plan_kernel(group, slots, levels, old_ref, new_ref, mine_ref, send_ref, pick_ref, count_ref, dst_ref, src_ref, rank_ref):
    layers, experts = old_ref.shape
    half = group // 2
    me = lax.axis_index("expert")
    my_half = lax.div(me, half)

    def clear(i, c):
        send_ref[i] = 0
        return c

    lax.fori_loop(0, layers * half, clear, 0)
    for layer in range(layers):

        def expert_step(e, c):
            old, new = old_ref[layer, e], new_ref[layer, e]

            @pl.when(old != new)
            def _():
                src, dst = lax.div(old, slots), lax.div(new, slots)
                dst_ref[layer * group + src] = dst
                src_ref[layer * group + dst] = src

                @pl.when(src == me)
                def _():
                    mine_ref[layer] = lax.rem(old, slots)

                @pl.when(dst == me)
                def _():
                    mine_ref[layers + layer] = lax.rem(new, slots)

            return c

        lax.fori_loop(0, experts, expert_step, 0)
    counts = [jnp.int32(0), jnp.int32(0)]
    for layer in range(layers):
        for side in range(2):

            def rank_step(j, count, side=side):
                at = layer * group + side * half + j
                crosses = lax.div(dst_ref[at], half) != side
                rank_ref[at] = count

                @pl.when(crosses & (my_half == side))
                def _():
                    send_ref[count] = layer * half + j

                return count + crosses.astype(jnp.int32)

            counts[side] = lax.fori_loop(0, half, rank_step, counts[side])
    count_ref[0] = sum((counts[0] > level).astype(jnp.int32) for level in levels[:-1])
    for layer in range(layers):

        def pick_step(j, c):
            src = src_ref[layer * group + my_half * half + j]
            local = lax.div(src, half) == my_half
            pick_ref[layer * half + j] = jnp.where(
                local,
                layer * half + lax.rem(src, half),
                layers * half + rank_ref[layer * group + src],
            )
            return c

        lax.fori_loop(0, half, pick_step, 0)


def make_plan(old_slot, new_slot, group, slots, levels):
    layers = old_slot.shape[0]
    half = group // 2
    smem = pl.BlockSpec(memory_space=pltpu.SMEM)
    i32 = lambda n: jax.ShapeDtypeStruct((n,), jnp.int32)
    return pl.pallas_call(
        functools.partial(plan_kernel, group, slots, levels),
        out_shape=(i32(2 * layers), i32(layers * half), i32(layers * half), i32(1)),
        in_specs=[smem, smem],
        out_specs=(smem, smem, smem, smem),
        scratch_shapes=[pltpu.SMEM((layers * group,), jnp.int32)] * 3,
    )(old_slot, new_slot)


def move_kernel(
    dims, mine_ref, send_ref, pick_ref, master_hbm, one_hbm, two_hbm, grad_hbm,
    land0, land1, land2, clip_ref, master_ref, one_ref, two_ref, grad_ref, src0, src1, src2,
    norm_dp, norm_ex, norm_a, norm_b, in_sem,
    a_send, a_recv, b_send, b_recv, c_send, c_recv, d_send, d_recv, e_send, e_recv, *bufs,
):
    group, dps, layers, slots, rows, cols, tiles, cuts, cap = dims
    half, hubs = group // 2, group // 4
    piece = cuts[-1]
    chunks = [(a, lo, hi) for a in range(3) for lo, hi in zip(cuts[:-1], cuts[1:])]
    count = len(chunks)
    hubbuf, fars, outs, gives = (bufs[i * count:(i + 1) * count] for i in range(4))
    lands, srcs = (land0, land1, land2), (src0, src1, src2)
    me, my_dp = lax.axis_index("expert"), lax.axis_index("dp")
    my_half = lax.div(me, half)
    base = my_half * half
    spot = lax.rem(me, half)
    first_hub = hubs + my_half * hubs
    is_hub = (me >= hubs) & (me < 3 * hubs)
    my_piece = lax.rem(me, hubs)
    partner = jnp.where(my_half == 0, me + hubs, me - hubs)
    col_tiles = -(-cols // LANE)

    loads = [
        pltpu.make_async_copy(src, dst, in_sem.at[i])
        for i, (src, dst) in enumerate(
            ((master_hbm, master_ref), (grad_hbm, grad_ref), (one_hbm, one_ref), (two_hbm, two_ref))
        )
    ]
    for load in loads:
        load.start()

    barrier = pltpu.get_barrier_semaphore()

    def greet(d, c):
        @pl.when(d != me)
        def _():
            pl.semaphore_signal(barrier, inc=1, device_id={"expert": d}, device_id_type=MESH)

        return c

    def greet_dp(d, c):
        @pl.when(d != my_dp)
        def _():
            pl.semaphore_signal(barrier, inc=1, device_id={"dp": d}, device_id_type=MESH)

        return c

    lax.fori_loop(0, group, greet, 0)
    lax.fori_loop(0, dps, greet_dp, 0)

    def padded(tile):
        if tile.shape[1] == LANE:
            return tile
        return jnp.concatenate([tile, jnp.zeros((SUB, LANE - tile.shape[1]), jnp.float32)], axis=1)

    def spans():
        for r in range(rows // SUB):
            for c in range(col_tiles):
                yield r * col_tiles + c, pl.ds(r * SUB, SUB), pl.ds(c * LANE, min(LANE, cols - c * LANE))

    loads[0].wait()
    for layer in range(layers):
        slot = mine_ref[layer]
        for t, rspan, cspan in spans():
            src0[layer, t] = padded(master_ref[layer, slot, rspan, cspan])
        for s in srcs:
            for t in range(tiles, piece * hubs):
                s[layer, t] = jnp.zeros((SUB, LANE), jnp.float32)

    pl.semaphore_wait(barrier, group + dps - 2)

    def a_copy(n, layer, p, slot):
        a, lo, hi = chunks[n]
        return pltpu.make_async_remote_copy(
            src_ref=srcs[a].at[layer, pl.ds(p * piece + lo, hi - lo)],
            dst_ref=hubbuf[n].at[layer * half + slot],
            send_sem=a_send.at[n, layer, p],
            recv_sem=a_recv.at[n, layer * half + slot],
            device_id={"expert": first_hub + p},
            device_id_type=MESH,
        )

    def a_start(n):
        a, lo, hi = chunks[n]
        for layer in range(layers):
            for p in range(hubs):
                mine = first_hub + p == me

                @pl.when(jnp.logical_not(mine))
                def _(layer=layer, p=p):
                    a_copy(n, layer, p, spot).start()

                @pl.when(mine)
                def _(layer=layer, p=p):
                    hubbuf[n][layer * half + spot] = srcs[a][layer, p * piece + lo:p * piece + hi]

    def a_wait_send(n):
        for layer in range(layers):
            for p in range(hubs):

                @pl.when(first_hub + p != me)
                def _(layer=layer, p=p):
                    a_copy(n, layer, p, spot).wait_send()

    def a_wait_recv(n):
        for layer in range(layers):

            def step(j, c, layer=layer):
                @pl.when(j != spot)
                def _():
                    a_copy(n, layer, 0, j).wait_recv()

                return c

            lax.fori_loop(0, half, step, 0)

    def b_copy(n):
        return pltpu.make_async_remote_copy(
            src_ref=outs[n], dst_ref=fars[n], send_sem=b_send.at[n], recv_sem=b_recv.at[n],
            device_id={"expert": partner}, device_id_type=MESH,
        )

    def b_start(n):
        def step(k, c):
            outs[n][k] = hubbuf[n][send_ref[k]]
            return c

        lax.fori_loop(0, cap, step, 0)
        b_copy(n).start()

    def landing(n, layer, p):
        a, lo, hi = chunks[n]
        return lands[a].at[layer, pl.ds(p * piece + lo, hi - lo)]

    def c_copy(n, layer, j, p):
        return pltpu.make_async_remote_copy(
            src_ref=gives[n].at[layer * half + j],
            dst_ref=landing(n, layer, p),
            send_sem=c_send.at[n, layer * half + j],
            recv_sem=c_recv.at[n, layer, p],
            device_id={"expert": base + j},
            device_id_type=MESH,
        )

    def c_start(n):
        for layer in range(layers):

            def step(j, c, layer=layer):
                code = pick_ref[layer * half + j]
                near = hubbuf[n][jnp.minimum(code, layers * half - 1)]
                far = fars[n][jnp.clip(code - layers * half, 0, cap - 1)]
                gives[n][layer * half + j] = jnp.where(code < layers * half, near, far)
                return c

            lax.fori_loop(0, half, step, 0)

        for layer in range(layers):

            def send(j, c, layer=layer):
                @pl.when(j != spot)
                def _():
                    c_copy(n, layer, j, my_piece).start()

                return c

            lax.fori_loop(0, half, send, 0)
            landing(n, layer, my_piece)[...] = gives[n][layer * half + spot]

    def c_wait_send(n):
        for layer in range(layers):

            def step(j, c, layer=layer):
                @pl.when(j != spot)
                def _():
                    c_copy(n, layer, j, my_piece).wait_send()

                return c

            lax.fori_loop(0, half, step, 0)

    def c_wait_recv(n):
        for layer in range(layers):
            for p in range(hubs):

                @pl.when(first_hub + p != me)
                def _(layer=layer, p=p):
                    c_copy(n, layer, 0, p).wait_recv()

    early = [n for n in range(count) if chunks[n][0] == 0]
    for n in early:
        a_start(n)

    loads[1].wait()
    parts = [jnp.zeros((rows, LANE), jnp.float32) for _ in range(4)]
    tails = jnp.zeros((rows, cols - (col_tiles - 1) * LANE), jnp.float32)
    for layer in range(layers):
        for s in range(slots):
            for c in range(col_tiles - 1):
                wide = grad_ref[layer, s, :, pl.ds(c * LANE, LANE)].astype(jnp.float32)
                parts[c % 4] = parts[c % 4] + wide * wide
            last = (col_tiles - 1) * LANE
            wide = grad_ref[layer, s, :, pl.ds(last, cols - last)].astype(jnp.float32)
            tails = tails + wide * wide
    square = jnp.sum((parts[0] + parts[1]) + (parts[2] + parts[3])) + jnp.sum(tails)

    def exchange(value, send_buf, box, axis, size, mine, send_sem, recv_sem):
        tile = jnp.full((SUB, LANE), value, jnp.float32)
        send_buf[...] = tile
        box[mine] = tile

        def copy(peer, slot):
            return pltpu.make_async_remote_copy(
                src_ref=send_buf, dst_ref=box.at[slot], send_sem=send_sem.at[peer],
                recv_sem=recv_sem.at[slot], device_id={axis: peer}, device_id_type=MESH,
            )

        def each(act):
            def step(d, c):
                @pl.when(d != mine)
                def _():
                    act(d)

                return c

            lax.fori_loop(0, size, step, 0)

        each(lambda d: copy(d, mine).start())
        each(lambda d: copy(d, d).wait_recv())
        each(lambda d: copy(d, mine).wait_send())
        total = box[0]
        for d in range(1, size):
            total = total + box[d]
        return total

    by_dp = exchange(square, norm_a, norm_dp, "dp", dps, my_dp, d_send, d_recv)
    total = exchange(by_dp, norm_b, norm_ex, "expert", group, me, e_send, e_recv)
    entry_count = layers * slots * group * rows * dps * cols
    clip = jnp.minimum(1.0, CLIP_RMS * math.sqrt(entry_count) / (jnp.sqrt(total) + 1e-06))
    clip_ref[...] = clip
    loads[2].wait()
    loads[3].wait()
    for layer in range(layers):
        slot = mine_ref[layer]
        for c in range(col_tiles):
            cspan = pl.ds(c * LANE, min(LANE, cols - c * LANE))
            wide = grad_ref[layer, slot, :, cspan].astype(jnp.float32)
            first, second = moments(
                one_ref[layer, slot, :, cspan], two_ref[layer, slot, :, cspan], wide, clip[0:1, 0:1]
            )
            for r in range(rows // SUB):
                src1[layer, r * col_tiles + c] = padded(first[r * SUB:(r + 1) * SUB])
                src2[layer, r * col_tiles + c] = padded(second[r * SUB:(r + 1) * SUB])
    for n in range(len(early), count):
        a_start(n)

    @pl.when(is_hub)
    def _():
        for n in range(count):
            a_wait_recv(n)
            b_start(n)
            if n:
                b_copy(n - 1).wait_recv()
                c_start(n - 1)
        b_copy(count - 1).wait_recv()
        c_start(count - 1)
        for n in range(count):
            b_copy(n).wait_send()
            c_wait_send(n)

    for n in range(count):
        a_wait_send(n)
        c_wait_recv(n)


def move_blocks(group, dps, cap, ident, mine, send, pick, master, moment_one, moment_two, gradient):
    layers, slots, rows, cols = master.shape
    half, hubs = group // 2, group // 4
    tiles = (rows // SUB) * -(-cols // LANE)
    piece = -(-tiles // hubs)
    cuts = tuple(sorted({0, piece // 3, piece * 2 // 3, piece}))
    dims = (group, dps, layers, slots, rows, cols, tiles, cuts, cap)
    smem = pl.BlockSpec(memory_space=pltpu.SMEM)
    hbm = pl.BlockSpec(memory_space=pltpu.HBM)
    vmem = pl.BlockSpec(memory_space=pltpu.VMEM)
    f32 = jnp.float32
    buf = lambda *lead: pltpu.VMEM(lead + (SUB, LANE), f32)
    dma = lambda *shape: pltpu.SemaphoreType.DMA(shape)
    land = jax.ShapeDtypeStruct((layers, piece * hubs, SUB, LANE), f32)
    widths = [hi - lo for lo, hi in zip(cuts[:-1], cuts[1:])] * 3
    count = len(widths)
    return pl.pallas_call(
        functools.partial(move_kernel, dims),
        out_shape=(land, land, land, jax.ShapeDtypeStruct((SUB, LANE), f32)),
        in_specs=[smem] * 3 + [hbm] * 4,
        out_specs=(vmem,) * 4,
        scratch_shapes=[pltpu.VMEM(master.shape, f32)] * 3
        + [pltpu.VMEM(gradient.shape, gradient.dtype)]
        + [buf(layers, piece * hubs)] * 3
        + [buf(dps), buf(group), buf(), buf()]
        + [dma(4)]
        + [dma(count, layers, hubs), dma(count, layers * half), dma(count), dma(count),
           dma(count, layers * half), dma(count, layers, hubs), dma(dps), dma(dps), dma(group), dma(group)]
        + [buf(layers * half, w) for w in widths]
        + [buf(cap, w) for w in widths] * 2
        + [buf(layers * half, w) for w in widths],
        compiler_params=pltpu.CompilerParams(
            collective_id=ident, has_side_effects=True, vmem_limit_bytes=40 * 1024 * 1024
        ),
    )(mine, send, pick, master, moment_one, moment_two, gradient)


def merge_kernel(
    mine_ref, master_hbm, one_hbm, two_hbm, grad_hbm, came0, came1, came2, clip_ref, w_hbm, f_hbm, s_hbm,
    master_ref, one_ref, two_ref, grad_ref, w_ref, f_ref, s_ref, in_sem, out_sem,
):
    layers, slots, rows, cols = master_ref.shape
    col_tiles = -(-cols // LANE)
    pairs = ((grad_hbm, grad_ref), (one_hbm, one_ref), (two_hbm, two_ref), (master_hbm, master_ref))
    blocks = layers * slots

    def read(i, n):
        layer, slot = lax.div(i, slots), lax.rem(i, slots)
        src, dst = pairs[n]
        return pltpu.make_async_copy(src.at[layer, slot], dst.at[layer, slot], in_sem.at[i, n])

    def write(i, n):
        layer, slot = lax.div(i, slots), lax.rem(i, slots)
        src, dst = ((w_ref, w_hbm), (f_ref, f_hbm), (s_ref, s_hbm))[n]
        return pltpu.make_async_copy(src.at[layer, slot], dst.at[layer, slot], out_sem.at[i, n])

    def begin(i, c):
        for n in range(4):
            read(i, n).start()
        return c

    lax.fori_loop(0, blocks, begin, 0)

    def step(i, c):
        layer, slot = lax.div(i, slots), lax.rem(i, slots)
        for n in range(4):
            read(i, n).wait()

        arrives = mine_ref[layers + layer] == slot

        @pl.when(jnp.logical_not(arrives))
        def _():
            scale = clip_ref[0:1, 0:1]
            for k in range(col_tiles):
                at = (layer, slot, slice(None), pl.ds(k * LANE, min(LANE, cols - k * LANE)))
                first, second = moments(one_ref[at], two_ref[at], grad_ref[at].astype(jnp.float32), scale)
                f_ref[at] = first
                s_ref[at] = second
                w_ref[at] = weights_of(master_ref[at], first, second)

        @pl.when(arrives)
        def _():
            for r in range(rows // SUB):
                for k in range(col_tiles):
                    t = r * col_tiles + k
                    width = min(LANE, cols - k * LANE)
                    at = (layer, slot, pl.ds(r * SUB, SUB), pl.ds(k * LANE, width))
                    first, second = came1[layer, t][:, :width], came2[layer, t][:, :width]
                    f_ref[at] = first
                    s_ref[at] = second
                    w_ref[at] = weights_of(came0[layer, t][:, :width], first, second)

        for n in range(3):
            write(i, n).start()
        return c

    lax.fori_loop(0, blocks, step, 0)

    def end(i, c):
        for n in range(3):
            write(i, n).wait()
        return c

    lax.fori_loop(0, blocks, end, 0)


def merge(mine, master, moment_one, moment_two, gradient, landed, clip):
    layers, slots = master.shape[:2]
    blocks = layers * slots
    smem = pl.BlockSpec(memory_space=pltpu.SMEM)
    hbm = pl.BlockSpec(memory_space=pltpu.HBM)
    vmem = pl.BlockSpec(memory_space=pltpu.VMEM)
    full = pltpu.VMEM(master.shape, jnp.float32)
    out = jax.ShapeDtypeStruct(master.shape, jnp.float32)
    dma = lambda *shape: pltpu.SemaphoreType.DMA(shape)
    return pl.pallas_call(
        merge_kernel,
        out_shape=(out, out, out),
        in_specs=[smem] + [hbm] * 4 + [vmem] * 4,
        out_specs=(hbm,) * 3,
        scratch_shapes=[full] * 3
        + [pltpu.VMEM(gradient.shape, gradient.dtype)]
        + [full] * 3
        + [dma(blocks, 4), dma(blocks, 3)],
        compiler_params=pltpu.CompilerParams(vmem_limit_bytes=40 * 1024 * 1024),
    )(mine, master, moment_one, moment_two, gradient, *landed, clip)


def shards(group, dps, master, moment_one, moment_two, gradient, old_slot, new_slot):
    layers, slots = master.shape[:2]
    full = layers * (group // 2)
    levels = sorted({-(-full * step // 8) for step in (3, 4, 5, 6, 8)})
    mine, send, pick, index = make_plan(old_slot, new_slot, group, slots, levels)
    moves = [
        functools.partial(move_blocks, group, dps, level, ident) for ident, level in enumerate(levels)
    ]
    *landed, clip = lax.switch(
        index[0], moves, mine, send, pick, master, moment_one, moment_two, gradient
    )
    return merge(mine, master, moment_one, moment_two, gradient, landed, clip)


def solution(mesh):
    split = P(None, "expert", "dp", None)
    body = functools.partial(shards, mesh.shape["expert"], mesh.shape["dp"])
    return jax.shard_map(
        body, mesh=mesh, in_specs=(split,) * 4 + (P(), P()), out_specs=(split,) * 3, check_vma=False
    )
```
